256 devices in a mesh: cen: 32 (over y_lo, z, core), out: 8 (over x, y_hi).
Axes of the slice: x: 4, y: 4 (y_hi: 2, y_lo: 2; y = y_hi * 2 + y_lo), z: 8, core: 2. Of those that a mesh axis runs over, the one named last changes fastest.
Arguments:
- features: float32 [65536, 1024], P('cen', 'out'), may hold values from -6 to 6
- centres: float32 [65536, 1024], P('cen', 'out'), may hold values from -6 to 6
- coefs: float32 [65536, 1000], P('cen', 'out'), may hold values from -0.046875 to 0.046875
- batch_index: int32 [2, 512], P(None, 'cen'), may hold values from 0 to 2047
- targets: float32 [2, 512, 1000], P(None, 'cen', 'out'), may hold values from -6 to 6
Outputs:
- residuals: float32 [2, 512, 1000], P(None, 'cen', 'out')
- new_coefs: float32 [65536, 1000], P('cen', 'out')
The draws below stay inside these ranges and needn't reach their ends.
All inputs are finite; a program needn't handle non-finite values.
Results may differ from the reference program's by a relative error of at most 0.0001.
Values sent between devices are 32-bit elements; how exact they have to be, the bound alone decides.
A program may use at most 64 MiB of HBM per device.

```python
import jax
import jax.numpy as jnp
from jax import lax

W = 1024
O = 1000
BAT_DEV = 16
P_DEV = 2048
CENTRES = 65536
BATCH = 512
POINTS = 65536


def scaled_rows(key, rows, cols):
    first, second = jax.random.split(key)
    base = jax.random.normal(first, (rows, cols), jnp.float32)
    scales = jnp.exp(jax.random.uniform(second, (rows, 1), jnp.float32, jnp.log(0.25), jnp.log(1.0)))
    return jnp.clip(base * scales, -6.0, 6.0)


def draw_features(key, part):
    return scaled_rows(jax.random.fold_in(key, 11), POINTS, W)


def draw_centres(key, part):
    return scaled_rows(jax.random.fold_in(key, 23), CENTRES, W)


def plant(entries, stream_key, smallest, largest):
    longest = entries.shape.index(max(entries.shape))
    spots = []
    for shift in (0, 1):
        where = [jax.random.randint(jax.random.fold_in(stream_key, axis), (), 0, length) for axis, length in enumerate(entries.shape)]
        where[longest] = (where[longest] + shift) % entries.shape[longest]
        spots.append(tuple(where))
    return entries.at[spots[0]].set(smallest).at[spots[1]].set(largest)


def levels(own_key, dims, pieces, least, largest):
    loudness = 1.0
    for dim, parts in pieces:
        draws = jax.random.uniform(jax.random.fold_in(jax.random.fold_in(own_key, 6), dim), (parts,), jnp.float32, least / len(pieces), largest / len(pieces))
        loudness = loudness * jnp.repeat(jnp.exp(draws), dims[dim] // parts).reshape((-1,) + (1,) * (len(dims) - 1 - dim))
    return loudness


def scatter_about(key, dims, scale, limit, pieces=(), held_as=jnp.bfloat16):
    gain = levels(key, dims, pieces, -0.22, 0.18) if pieces else 1.0
    drawn = jax.random.normal(key, dims, jnp.float32) * scale * gain
    return jnp.minimum(jnp.maximum(drawn, -limit), limit).astype(held_as)


def setup_inputs(seed: int = 0) -> dict:
    splits = jax.random.split(jax.random.key(seed), 6)
    return {
        "features": draw_features(jax.random.fold_in(splits[5], 71), 0),
        "centres": draw_centres(jax.random.fold_in(splits[5], 71), 0),
        "coefs": scatter_about(splits[2], (CENTRES, O), (CENTRES // 4) ** -0.5, 0.046875, ((0, 32), (1, 8)), jnp.float32),
        "batch_index": plant(jax.random.randint(splits[3], (2, BATCH), 0, P_DEV), jax.random.fold_in(splits[3], 1), 0, P_DEV - 1).astype(jnp.int32),
        "targets": scatter_about(splits[4], (2, BATCH, O), 1.0, 6.0, ((1, 32), (2, 8)), jnp.float32),
    }


def kernel_rows(batch, centres):
    batch_sq = lax.optimization_barrier(jnp.sum(batch * batch, axis=1))
    centre_sq = lax.optimization_barrier(jnp.sum(centres * centres, axis=1))
    inner = lax.dot_general(batch, centres, (((1,), (1,)), ((), ())), precision=lax.Precision.HIGHEST, preferred_element_type=jnp.float32)
    squared = batch_sq[:, None] + centre_sq[None, :] - 2.0 * inner
    return jnp.exp(-jnp.sqrt(jnp.maximum(squared, 0.0)) / (0.5 * jnp.sqrt(jnp.float32(W))))

def reference(features, centres, coefs, batch_index, targets):
    owner = jnp.arange(BATCH, dtype=jnp.int32) // BAT_DEV * P_DEV
    new_coefs = coefs
    results = []
    for step in range(2):
        rows = features[owner + batch_index[step]]
        kern = kernel_rows(rows, centres)
        predict = jnp.dot(kern, coefs, precision=lax.Precision.HIGHEST, preferred_element_type=jnp.float32)
        resid = predict - targets[step]
        results.append(resid)
        grad = lax.dot_general(kern, resid, (((0,), (0,)), ((), ())), precision=lax.Precision.HIGHEST, preferred_element_type=jnp.float32) / BATCH
        scale = jnp.sqrt(jnp.sum(grad * grad) / (CENTRES * O) + 1e-06)
        new_coefs = new_coefs - 0.1 * grad / scale
    return (jnp.stack(results), new_coefs)
```

```python
import functools
import math

import jax
import jax.numpy as jnp
from jax import lax
from jax.experimental import pallas as pl
from jax.experimental.pallas import tpu as pltpu
from jax.sharding import Mesh
from jax.sharding import PartitionSpec as P

W = 1024
LANES = 128
CEN = ("cen_0", "cen_1", "cen_2")
OUT = ("out_0", "out_1")
MESH = pl.DeviceIdType.MESH
NX, NY, NZ = 4, 4, 8
F32, BF16 = jnp.float32, jnp.bfloat16


def halves(v):
    hi = v.astype(BF16)
    return hi, (v - hi.astype(F32)).astype(BF16)


def dot_rows(a, b):
    return lax.dot_general(a, b, (((1,), (1,)), ((), ())), preferred_element_type=F32)


def dot_plain(a, b):
    return lax.dot_general(a, b, (((1,), (0,)), ((), ())), preferred_element_type=F32)


def kernel(
    entries, idx_ref, feat_ref, cen_ref, coef_ref, targ_ref, upd_ref, res_ref,
    cpad, bs, cs, gs, chi, clo, ghi, glo, sbh, sbl, kf, kth, ktl,
    psend, precv, q, rx0, s0, ry0, ry1, t1, rx1, tz, rz, rb, rhi, rlo,
    g, us, pv, pd, pz, pp,
    pl_s, pl_r, cx_s, cx_r, cy_s, cy_r, gx_s, gx_r, z_s, z_r, d_s, d_r,
    pr_s, pr_r, x0_s, x0_r, y0_s, y0_r, y1_s, y1_r, x1_s, x1_r, rz_s, rz_r,
    az_s, az_r, ay0_s, ay0_r, ax0_s, ax0_r, ax1_s, ax1_r, ay1_s, ay1_r, ad_s, ad_r,
    p_s, p_r, u_s, u_r,
):
    x, yh = lax.axis_index("out_0"), lax.axis_index("out_1")
    yl, z, c = lax.axis_index("cen_0"), lax.axis_index("cen_1"), lax.axis_index("cen_2")
    y = yh * 2 + yl
    rows = cen_ref.shape[0] // NX
    blk = yh * NX + x

    def at_x(d):
        return lax.rem(x + d, NX)

    def at_z(d):
        return lax.rem(z + d + NZ, NZ)

    def to(dx=0, dy=0, dz=0, flip=False):
        ny = lax.rem(y + dy, NY)
        return {
            "out_0": at_x(dx), "out_1": lax.div(ny, 2), "cen_0": lax.rem(ny, 2),
            "cen_1": at_z(dz), "cen_2": 1 - c if flip else c,
        }

    pair_y = {"out_0": x, "out_1": yh, "cen_0": 1 - yl, "cen_1": z, "cen_2": c}
    plane = [(dx, dy) for dx in range(NX) for dy in range(NY) if dx or dy]
    peers = [to(dx, dy) for dx, dy in plane] + [to(dz=d) for d in range(1, NZ)] + [to(flip=True)]

    barrier = pltpu.get_barrier_semaphore()
    for peer in peers:
        pl.semaphore_signal(barrier, inc=1, device_id=peer, device_id_type=MESH)

    sent = []

    def send(src, dst, ss, rs, dev):
        copy = pltpu.make_async_remote_copy(
            src_ref=src, dst_ref=dst, send_sem=ss, recv_sem=rs, device_id=dev, device_id_type=MESH
        )
        copy.start()
        sent.append(copy)
        return copy

    mine = bs.at[z, c, yl, blk]
    for k in range(2):
        for j in range(16):
            mine[pl.ds(k * 16 + j, 1), :] = feat_ref[pl.ds(idx_ref[k, j], 1), :]
    cs[blk] = cen_ref[pl.ds(pl.multiple_of(x * rows, 8), rows), :]
    wide = coef_ref.shape[1]

    @pl.loop(0, cpad.shape[0] // 256)
    def _(i):
        at = pl.ds(pl.multiple_of(i * 256, 256), 256)
        cpad[at, :] = jnp.zeros((256, LANES), F32)
        cpad[at, pl.ds(0, wide)] = coef_ref[at, :]

    gs[x] = cpad[pl.ds(pl.multiple_of(x * rows, 8), rows), :]
    pl.semaphore_wait(barrier, len(peers))

    got_plane = [
        send(mine, mine, pl_s.at[n], pl_r.at[n], to(dx, dy)) for n, (dx, dy) in enumerate(plane)
    ]
    got_cx = {}
    for d in (2, 1, 3):
        src = cen_ref.at[pl.ds(pl.multiple_of(at_x(d) * rows, 8), rows)]
        got_cx[d] = send(src, cs.at[blk], cx_s.at[d - 1], cx_r.at[d - 1], to(dx=d))
    own = cen_ref.at[pl.ds(pl.multiple_of(x * rows, 8), rows)]
    got_cy = {0: send(own, cs.at[blk], cy_s.at[0], cy_r.at[0], to(dy=2))}

    for copy in got_plane:
        copy.wait_recv()
    got_z, got_d = {}, {}
    for h in range(2):
        part = bs.at[z, c, h]
        for way, dz in ((0, 1), (1, -1)):
            got_z[way, 1, h] = send(part, part, z_s.at[way, 0, h], z_r.at[way, 0, h], to(dz=dz))
    for h in range(2):
        part = bs.at[z, c, h]
        got_d[0, h] = send(part, part, d_s.at[0, h], d_r.at[0, h], to(flip=True))

    for d in (1, 3, 2):
        got_cx[d].wait_recv()
        part = cs.at[yh * NX + at_x(NX - d)]
        got_cy[d] = send(part, part, cy_s.at[d], cy_r.at[d], to(dy=2))
    got_g = []
    for d in range(1, NX):
        src = cpad.at[pl.ds(pl.multiple_of(at_x(d) * rows, 8), rows)]
        got_g.append(send(src, gs.at[x], gx_s.at[d - 1], gx_r.at[d - 1], to(dx=d)))

    def ring_step(s):
        for h in range(2):
            for way, dz in ((0, 1), (1, -1)):
                if s == 4 and h != way:
                    continue
                got_z[way, s, h].wait_recv()
                part = bs.at[at_z(-dz * s), c, h]
                if s < 3 or (s == 3 and h == way):
                    got_z[way, s + 1, h] = send(
                        part, part, z_s.at[way, s, h], z_r.at[way, s, h], to(dz=dz)
                    )
                rel = (-dz * s) % NZ
                got_d[rel, h] = send(part, part, d_s.at[rel, h], d_r.at[rel, h], to(flip=True))

    def take_centres(base):
        for i in range(NX):
            v = cs[base + i]
            hi, lo = halves(v)
            at = pl.ds(pl.multiple_of((base + i) * LANES, LANES), LANES)
            chi[:, at] = hi
            clo[:, at] = lo

    take_centres(yh * NX)
    ring_step(1)
    ring_step(2)
    ring_step(3)
    for d in range(NX):
        got_cy[d].wait_recv()
    take_centres((1 - yh) * NX)
    total = cs[0] * cs[0]
    for i in range(1, 2 * NX):
        total = total + cs[i] * cs[i]
    centre_sq = jnp.sum(total.T, axis=0, keepdims=True)

    def kernel_slab(rel):
        zs = at_z(rel)
        for h in range(2):
            got_d[rel, h].wait_recv()
        squares = []
        for cc in range(2):
            for h in range(2):
                at = pl.ds((cc * 2 + h) * 32, 32)
                acc = None
                for b in range(2 * NX):
                    v = bs[zs, cc, h, b]
                    hi, lo = halves(v)
                    sbh[at, pl.ds(b * LANES, LANES)] = hi
                    sbl[at, pl.ds(b * LANES, LANES)] = lo
                    acc = v * v if acc is None else acc + v * v
                squares.append(jnp.sum(acc, axis=1, keepdims=True))
        batch_sq = jnp.concatenate(squares, axis=0)
        bh, bl = sbh[...], sbl[...]
        for n in range(rows // 256):
            cat = pl.ds(n * 256, 256)
            ch, cl = chi[cat, :], clo[cat, :]
            inner = (dot_rows(bl, cl) + dot_rows(bl, ch)) + dot_rows(bh, cl) + dot_rows(bh, ch)
            sq = batch_sq + centre_sq[:, n * 256 : (n + 1) * 256] - 2.0 * inner
            kern = jnp.exp(jnp.sqrt(jnp.maximum(sq, 0.0)) * (-1.0 / (0.5 * math.sqrt(W))))
            for cc in range(2):
                for h in range(2):
                    for k in range(2):
                        r = (cc * 2 + h) * 32 + k * 16
                        kf[k, cc, h, pl.ds(pl.multiple_of(zs * 16, 16), 16), cat] = kern[r : r + 16]

    for rel in (0, 1, 7, 2, 6, 3, 5):
        kernel_slab(rel)
    for copy in got_g:
        copy.wait_recv()
    for i in range(NX):
        hi, lo = halves(gs[i])
        ghi[:, pl.ds(i * LANES, LANES)] = hi
        glo[:, pl.ds(i * LANES, LANES)] = lo
    ring_step(4)
    kernel_slab(4)

    def predict(k, cc, h):
        kh, kl = halves(kf[k, cc, h])
        return dot_plain(kl, ghi[...]) + dot_plain(kh, glo[...]) + dot_plain(kh, ghi[...])

    got_p = {}
    for k in (1, 0):
        for h in range(2):
            out = predict(k, 1 - c, h)
            for i in range(NX):
                psend[k, i, h] = out[:, i * LANES : (i + 1) * LANES]
        got_p[k] = send(psend.at[k], precv.at[k], pr_s.at[k], pr_r.at[k], to(flip=True))
    for k in (1, 0):
        for h in range(2):
            out = predict(k, c, h)
            for i in range(NX):
                q[k, i, h] = out[:, i * LANES : (i + 1) * LANES]

    def join(k):
        got_p[k].wait_recv()
        for i in range(NX):
            for h in range(2):
                q[k, i, h] = q[k, i, h] + precv[k, i, h]

    join(1)
    got_y1 = send(q.at[1, :, 1 - yl], ry1, y1_s.at[0], y1_r.at[0], pair_y)
    join(0)
    got_x0 = [
        send(q.at[0, at_x(d)], rx0.at[d - 1], x0_s.at[d - 1], x0_r.at[d - 1], to(dx=d))
        for d in (2, 1, 3)
    ]
    for k in range(2):
        for cc in range(2):
            for h in range(2):
                for n in range(rows // 128):
                    hi, lo = halves(kf[k, cc, h, :, pl.ds(n * 128, 128)].T)
                    at = pl.ds((cc * 2 + h) * 128, 128)
                    kth[k, pl.ds(n * 128, 128), at] = hi
                    ktl[k, pl.ds(n * 128, 128), at] = lo
    got_y1.wait_recv()
    for i in range(NX):
        t1[i] = q[1, i, yl] + ry1[i]
    got_x1 = [
        send(t1.at[at_x(d)], rx1.at[d - 1], x1_s.at[d - 1], x1_r.at[d - 1], to(dx=d))
        for d in (2, 1, 3)
    ]
    for copy in got_x0:
        copy.wait_recv()
    for h in range(2):
        s0[h] = (q[0, x, h] + rx0[0, h]) + (rx0[1, h] + rx0[2, h])
    got_y0 = send(s0.at[1 - yl], ry0, y0_s.at[0], y0_r.at[0], pair_y)

    def spread_z(k):
        return [
            send(tz.at[k, at_z(d)], rz.at[k, d - 1], rz_s.at[k, d - 1], rz_r.at[k, d - 1], to(dz=d))
            for d in range(1, NZ)
        ]

    for copy in got_x1:
        copy.wait_recv()
    tz[1] = ((t1[x] + rx1[0]) + (rx1[1] + rx1[2])).reshape(NZ, 16, LANES)
    got_z1 = spread_z(1)
    got_y0.wait_recv()
    tz[0] = (s0[yl] + ry0[...]).reshape(NZ, 16, LANES)
    got_z0 = spread_z(0)

    def residual(k, got):
        for copy in got:
            copy.wait_recv()
        acc = tz[k, z]
        for d in range(1, NZ):
            acc = acc + rz[k, d - 1]
        at = pl.ds(pl.multiple_of(z * 16, 16), 16)
        rb[k, x, c, yl, at, :] = jnp.zeros((16, LANES), F32)
        rb[k, x, c, yl, at, pl.ds(0, wide)] = acc[:, :wide] - targ_ref[k]
        block = rb.at[k, x, c, yl, at]
        res_ref[k] = block[...]
        return [
            send(block, block, az_s.at[k, d - 1], az_r.at[k, d - 1], to(dz=d)) for d in range(1, NZ)
        ]

    got_a1 = residual(1, got_z1)
    got_a0 = residual(0, got_z0)

    for copy in got_a1:
        copy.wait_recv()
    part = rb.at[1, x, c, yl]
    got_ax1 = [send(part, part, ax1_s.at[d - 1], ax1_r.at[d - 1], to(dx=d)) for d in (2, 1, 3)]
    for copy in got_a0:
        copy.wait_recv()
    part = rb.at[0, x, c, yl]
    got_ay0 = send(part, part, ay0_s.at[0], ay0_r.at[0], pair_y)
    for copy in got_ax1:
        copy.wait_recv()
    part = rb.at[1, :, c, yl]
    got_ay1 = send(part, part, ay1_s.at[0], ay1_r.at[0], pair_y)
    got_ad = {1: [], 0: []}
    got_ad[1].append(send(part, part, ad_s.at[0], ad_r.at[0], to(flip=True)))
    got_ay0.wait_recv()
    part = rb.at[0, x, c]
    got_ax0 = {
        d: send(part, part, ax0_s.at[d - 1], ax0_r.at[d - 1], to(dx=d)) for d in (2, 1, 3)
    }
    got_ad[0].append(send(part, part, ad_s.at[1], ad_r.at[1], to(flip=True)))
    for d in (1, 3, 2):
        got_ax0[d].wait_recv()
        part = rb.at[0, at_x(NX - d), c]
        got_ad[0].append(send(part, part, ad_s.at[1 + d], ad_r.at[1 + d], to(flip=True)))
    got_ay1.wait_recv()
    part = rb.at[1, :, c, 1 - yl]
    got_ad[1].append(send(part, part, ad_s.at[5], ad_r.at[5], to(flip=True)))

    def gradient(k):
        for copy in got_ad[k]:
            copy.wait_recv()
        for i in range(NX):
            for cc in range(2):
                for h in range(2):
                    hi, lo = halves(rb[k, i, cc, h])
                    at = pl.ds((cc * 2 + h) * 128, 128)
                    rhi[at, pl.ds(i * LANES, LANES)] = hi
                    rlo[at, pl.ds(i * LANES, LANES)] = lo
        acc = jnp.zeros((8, LANES), F32)
        for n in range(rows // 128):
            at = pl.ds(n * 128, 128)
            kh, kl = kth[k, at, :], ktl[k, at, :]
            out = dot_plain(kl, rhi[...]) + dot_plain(kh, rlo[...]) + dot_plain(kh, rhi[...])
            out = out * (1.0 / (2 * NZ * 2 * 16))
            for i in range(NX):
                v = out[:, i * LANES : (i + 1) * LANES]
                g[k, i, at, :] = v
                acc = acc + jnp.sum((v * v).reshape(16, 8, LANES), axis=0)
        pv[k] = acc

    gradient(0)
    gradient(1)

    got = send(pv, pd, p_s.at[0], p_r.at[0], to(flip=True))
    got.wait_recv()
    pz[...] = pv[...] + pd[...]
    acc = pz[...]
    got = [
        send(pz, pp.at[d], p_s.at[d], p_r.at[d], to(dz=d)) for d in range(1, NZ)
    ]
    for d, copy in enumerate(got, 1):
        copy.wait_recv()
        acc = acc + pp[d]
    pp[0] = acc
    got = [
        send(pp.at[0], pp.at[8 + n], p_s.at[8 + n], p_r.at[8 + n], to(dx, dy))
        for n, (dx, dy) in enumerate(plane)
    ]
    for n, copy in enumerate(got):
        copy.wait_recv()
        acc = acc + pp[8 + n]
    factor = []
    for k in range(2):
        sums = jnp.sum(jnp.sum(acc[k], axis=0, keepdims=True), axis=1, keepdims=True)
        factor.append(0.1 / jnp.sqrt(sums / entries + 1e-6))

    got = []
    for d in (2, 1, 3):
        us[d - 1] = g[0, at_x(d)] * factor[0] + g[1, at_x(d)] * factor[1]
        here = upd_ref.at[pl.ds(pl.multiple_of(x * rows, 8), rows)]
        got.append(send(us.at[d - 1], here, u_s.at[d - 1], u_r.at[d - 1], to(dx=d)))
    upd_ref[pl.ds(pl.multiple_of(x * rows, 8), rows), :] = g[0, x] * factor[0] + g[1, x] * factor[1]
    for copy in got:
        copy.wait_recv()
    for copy in sent:
        copy.wait_send()


def body(features, centres, coefs, batch_index, targets):
    total = centres.shape[0]
    rows = total // NX
    entries = total * lax.axis_size(CEN) * coefs.shape[1] * lax.axis_size(OUT)
    vm = lambda *shape: pltpu.VMEM(shape, F32)
    vb = lambda *shape: pltpu.VMEM(shape, BF16)
    dma = lambda *shape: pltpu.SemaphoreType.DMA(shape)
    two = lambda *shape: [dma(*shape), dma(*shape)]
    scratch = [
        vm(total, LANES), vm(8, 2, 2, 8, 32, LANES), vm(8, rows, LANES), vm(NX, rows, LANES),
        vb(rows, W), vb(rows, W), vb(rows, 512), vb(rows, 512), vb(128, W), vb(128, W),
        vm(2, 2, 2, 128, rows), vb(2, rows, 512), vb(2, rows, 512),
        vm(2, NX, 2, 128, LANES), vm(2, NX, 2, 128, LANES), vm(2, NX, 2, 128, LANES),
        vm(3, 2, 128, LANES), vm(2, 128, LANES), vm(128, LANES), vm(NX, 128, LANES),
        vm(NX, 128, LANES), vm(3, 128, LANES), vm(2, NZ, 16, LANES), vm(2, 7, 16, LANES),
        vm(2, NX, 2, 2, 128, LANES), vb(512, 512), vb(512, 512),
        vm(2, NX, rows, LANES), vm(3, rows, LANES),
        vm(2, 8, LANES), vm(2, 8, LANES), vm(2, 8, LANES), vm(23, 2, 8, LANES),
        *two(15), *two(3), *two(4), *two(3), *two(2, 4, 2), *two(8, 2),
        *two(2), *two(3), *two(1), *two(1), *two(3), *two(2, 7),
        *two(2, 7), *two(1), *two(3), *two(3), *two(1), *two(6),
        *two(23), *two(3),
    ]
    whole = pl.BlockSpec(memory_space=pltpu.VMEM)
    upd, resid = pl.pallas_call(
        functools.partial(kernel, float(entries)),
        out_shape=(
            jax.ShapeDtypeStruct((total, LANES), F32),
            jax.ShapeDtypeStruct((2, 16, LANES), F32),
        ),
        in_specs=[pl.BlockSpec(memory_space=pltpu.SMEM)] + [whole] * 4,
        out_specs=(whole, whole),
        scratch_shapes=scratch,
        compiler_params=pltpu.CompilerParams(
            collective_id=0, has_side_effects=True, vmem_limit_bytes=60 * 2**20
        ),
        name="step",
    )(batch_index, features, centres, coefs, targets)
    wide = coefs.shape[1]
    return resid[:, :, :wide], coefs - upd[:, :wide]


def solution(mesh):
    torus = Mesh(mesh.devices.reshape(2, 8, 2, 4, 2), ("cen_0", "cen_1", "cen_2", "out_0", "out_1"))
    return jax.shard_map(
        body,
        mesh=torus,
        in_specs=(P(CEN, OUT), P(CEN, OUT), P(CEN, OUT), P(None, CEN), P(None, CEN, OUT)),
        out_specs=(P(None, CEN, OUT), P(CEN, OUT)),
        check_vma=False,
    )
```

```python
import functools
import math

import jax
import jax.numpy as jnp
from jax import lax
from jax.experimental import pallas as pl
from jax.experimental.pallas import tpu as pltpu
from jax.sharding import Mesh
from jax.sharding import PartitionSpec as P

W = 1024
LANES = 128
CEN = ("cen_0", "cen_1", "cen_2")
OUT = ("out_0", "out_1")
MESH = pl.DeviceIdType.MESH
NX, NY, NZ = 4, 4, 8
F32, BF16 = jnp.float32, jnp.bfloat16


def halves(v):
    hi = v.astype(BF16)
    return hi, (v - hi.astype(F32)).astype(BF16)


def dot_rows(a, b):
    return lax.dot_general(a, b, (((1,), (1,)), ((), ())), preferred_element_type=F32)


def dot_plain(a, b):
    return lax.dot_general(a, b, (((1,), (0,)), ((), ())), preferred_element_type=F32)


EARLY = 224


def kernel(
    entries, idx_ref, feat_hbm, cen_hbm, coef_hbm, targ_hbm, new_hbm, res_ref,
    feat_ref, cen_ref, coef_ref, targ_ref,
    cpad, bs, cs, gs, cth, ctl, ghi, glo, sbh, sbl, bsq, kf, kth, ktl,
    po, psend, precv, q, rx0, s0, ry0, ry1, t1, rx1, tz, rz, rb, rhi, rlo,
    g, us, upd, e0, e1, pp,
    in_s, pl_s, pl_r, cx_s, cx_r, cy_s, cy_r, gx_s, gx_r, z_s, z_r, d_s, d_r,
    pr_s, pr_r, x0_s, x0_r, y0_s, y0_r, y1_s, y1_r, x1_s, x1_r, rz_s, rz_r,
    az_s, az_r, ay0_s, ay0_r, ax0_s, ax0_r, ax1_s, ax1_r, ay1_s, ay1_r, ad_s, ad_r,
    p_s, p_r, u_s, u_r, e_s, e_r, out_s,
):
    x, yh = lax.axis_index("out_0"), lax.axis_index("out_1")
    yl, z, c = lax.axis_index("cen_0"), lax.axis_index("cen_1"), lax.axis_index("cen_2")
    y = yh * 2 + yl
    rows = cen_ref.shape[0] // NX
    blk = yh * NX + x
    wide = coef_ref.shape[1]

    def at_x(d):
        return lax.rem(x + d, NX)

    def at_z(d):
        return lax.rem(z + d + NZ, NZ)

    def slot(i):
        return pl.ds(pl.multiple_of(i * rows, 8), rows)

    def lanes(i):
        return pl.ds(i * LANES, LANES)

    def to(dx=0, dy=0, dz=0, flip=False):
        ny = lax.rem(y + dy, NY)
        return {
            "out_0": at_x(dx), "out_1": lax.div(ny, 2), "cen_0": lax.rem(ny, 2),
            "cen_1": at_z(dz), "cen_2": 1 - c if flip else c,
        }

    pair_y = {"out_0": x, "out_1": yh, "cen_0": 1 - yl, "cen_1": z, "cen_2": c}
    plane = [(dx, dy) for dx in range(NX) for dy in range(NY) if dx or dy]
    peers = [to(dx, dy) for dx, dy in plane] + [to(dz=d) for d in range(1, NZ)] + [to(flip=True)]

    loads = [
        pltpu.make_async_copy(src, dst, in_s.at[n])
        for n, (src, dst) in enumerate(
            ((feat_hbm, feat_ref), (cen_hbm, cen_ref), (coef_hbm, coef_ref), (targ_hbm, targ_ref))
        )
    ]
    for load in loads:
        load.start()
    barrier = pltpu.get_barrier_semaphore()
    for peer in peers:
        pl.semaphore_signal(barrier, inc=1, device_id=peer, device_id_type=MESH)

    sent = []

    def send(src, dst, ss, rs, dev):
        copy = pltpu.make_async_remote_copy(
            src_ref=src, dst_ref=dst, send_sem=ss, recv_sem=rs, device_id=dev, device_id_type=MESH
        )
        copy.start()
        sent.append(copy)
        return copy

    mine = bs.at[z, c, yl, blk]
    loads[0].wait()
    for k in range(2):
        for j in range(16):
            mine[pl.ds(k * 16 + j, 1), :] = feat_ref[pl.ds(idx_ref[k, j], 1), :]
    loads[1].wait()
    cs[blk] = cen_ref[slot(x), :]
    pl.semaphore_wait(barrier, len(peers))

    got_plane = [
        send(mine, mine, pl_s.at[n], pl_r.at[n], to(dx, dy)) for n, (dx, dy) in enumerate(plane)
    ]
    got_cx = {}
    for d in (2, 1, 3):
        got_cx[d] = send(
            cen_ref.at[slot(at_x(d))], cs.at[blk], cx_s.at[d - 1], cx_r.at[d - 1], to(dx=d)
        )
    got_cy = {0: send(cen_ref.at[slot(x)], cs.at[blk], cy_s.at[0], cy_r.at[0], to(dy=2))}

    loads[2].wait()
    loads[3].wait()

    @pl.loop(0, cpad.shape[0] // 256)
    def _(i):
        at = pl.ds(pl.multiple_of(i * 256, 256), 256)
        cpad[at, :] = jnp.zeros((256, LANES), F32)
        cpad[at, pl.ds(0, wide)] = coef_ref[at, :]

    gs[x] = cpad[slot(x), :]

    for copy in got_plane:
        copy.wait_recv()
    got_z, got_d = {}, {}
    for h in range(2):
        part = bs.at[z, c, h]
        for way, dz in ((0, 1), (1, -1)):
            got_z[way, 1, h] = send(part, part, z_s.at[way, 0, h], z_r.at[way, 0, h], to(dz=dz))
    for h in range(2):
        part = bs.at[z, c, h]
        got_d[0, h] = send(part, part, d_s.at[0, h], d_r.at[0, h], to(flip=True))

    def split_rows(zs, cc, h):
        acc = [None, None]
        for b in range(2 * NX):
            for k in range(2):
                v = bs[zs, cc, h, b, pl.ds(k * 16, 16), :]
                hi, lo = halves(v)
                at = pl.ds(pl.multiple_of((k * 4 + cc * 2 + h) * 16, 16), 16)
                sbh[zs, at, lanes(b)] = hi
                sbl[zs, at, lanes(b)] = lo
                acc[k] = v * v if acc[k] is None else acc[k] + v * v
        for k in range(2):
            at = pl.ds(pl.multiple_of((k * 4 + cc * 2 + h) * 16, 16), 16)
            total = jnp.sum(acc[k], axis=1, keepdims=True)
            bsq[zs, at, :] = jnp.broadcast_to(total, (16, LANES))

    def other(rel):
        for h in range(2):
            got_d[rel, h].wait_recv()
            split_rows(at_z(rel), 1 - c, h)

    for h in range(2):
        split_rows(z, c, h)
    for d in (1, 3, 2):
        got_cx[d].wait_recv()
        part = cs.at[yh * NX + at_x(NX - d)]
        got_cy[d] = send(part, part, cy_s.at[d], cy_r.at[d], to(dy=2))
    got_g = [
        send(cpad.at[slot(at_x(d))], gs.at[x], gx_s.at[d - 1], gx_r.at[d - 1], to(dx=d))
        for d in (2, 1, 3)
    ]

    def ring_step(s):
        for h in range(2):
            for way, dz in ((0, 1), (1, -1)):
                if s == 4 and h != way:
                    continue
                got_z[way, s, h].wait_recv()
                part = bs.at[at_z(-dz * s), c, h]
                if s < 3 or (s == 3 and h == way):
                    got_z[way, s + 1, h] = send(
                        part, part, z_s.at[way, s, h], z_r.at[way, s, h], to(dz=dz)
                    )
                rel = (-dz * s) % NZ
                got_d[rel, h] = send(part, part, d_s.at[rel, h], d_r.at[rel, h], to(flip=True))
        for h in range(2):
            for way, dz in ((0, 1), (1, -1)):
                if s < 4 or h == way:
                    split_rows(at_z(-dz * s), c, h)

    def take_centres(base):
        squares = None
        for i in range(NX):
            v = cs[base + i].T
            hi, lo = halves(v)
            at = pl.ds(pl.multiple_of((base + i) * LANES, LANES), LANES)
            cth[at, :] = hi
            ctl[at, :] = lo
            squares = v * v if squares is None else squares + v * v
        return jnp.sum(squares, axis=0, keepdims=True)

    first_sq = take_centres(yh * NX)
    ring_step(1)
    other(0)
    ring_step(2)
    other(1)
    other(7)
    ring_step(3)
    other(2)
    other(6)
    for d in (0, 1, 3, 2):
        got_cy[d].wait_recv()
    centre_sq = first_sq + take_centres((1 - yh) * NX)

    def kernel_slab(rel):
        zs = at_z(rel)
        bh, bl = sbh[zs], sbl[zs]
        square = bsq[zs]
        for n in range(rows // 256):
            cat = pl.ds(n * 256, 256)
            ch, cl = cth[:, cat], ctl[:, cat]
            inner = (dot_plain(bl, cl) + dot_plain(bl, ch)) + dot_plain(bh, cl) + dot_plain(bh, ch)
            for i in range(2):
                lo = i * LANES
                sums = square + centre_sq[:, n * 256 + lo : n * 256 + lo + LANES]
                sq = sums - 2.0 * inner[:, lo : lo + LANES]
                kern = jnp.exp(jnp.sqrt(jnp.maximum(sq, 0.0)) * (-1.0 / (0.5 * math.sqrt(W))))
                for k in range(2):
                    at = pl.ds(pl.multiple_of(zs * 64, 64), 64)
                    kf[k, at, pl.ds(n * 256 + lo, LANES)] = kern[k * 64 : k * 64 + 64]

    got_p = {}

    def predict_slab(rel):
        zs = at_z(rel)
        at = pl.ds(pl.multiple_of(zs * 64, 64), 64)
        kh, kl = halves(jnp.concatenate([kf[0, at, :], kf[1, at, :]], axis=0))
        out = dot_plain(kl, ghi[...]) + dot_plain(kh, glo[...]) + dot_plain(kh, ghi[...])
        po[...] = out.reshape(2, 2, 2, 16, NX * LANES)
        zat = pl.ds(pl.multiple_of(zs * 16, 16), 16)
        for k in range(2):
            for h in range(2):
                for i in range(NX):
                    psend[zs, k, i, h] = po[k, 1 - c, h, :, lanes(i)]
        for k in range(2):
            for h in range(2):
                for i in range(NX):
                    q[k, i, h, zat, :] = po[k, c, h, :, lanes(i)]
        got_p[rel] = send(psend.at[zs], precv.at[zs], pr_s.at[rel], pr_r.at[rel], to(flip=True))

    def join(rel):
        got_p[rel].wait_recv()
        zs = at_z(rel)
        zat = pl.ds(pl.multiple_of(zs * 16, 16), 16)
        for k in range(2):
            for h in range(2):
                for i in range(NX):
                    q[k, i, h, zat, :] = q[k, i, h, zat, :] + precv[zs, k, i, h]

    for rel in (0, 1, 7, 2, 6):
        kernel_slab(rel)
    for copy in got_g:
        copy.wait_recv()
    for i in range(NX):
        hi, lo = halves(gs[i])
        ghi[:, lanes(i)] = hi
        glo[:, lanes(i)] = lo
    for rel in (3, 5):
        other(rel)
        kernel_slab(rel)
    ready = (0, 1, 7, 2, 6, 3, 5)
    for rel in ready:
        predict_slab(rel)
    ring_step(4)
    for rel in ready[:-2]:
        join(rel)
    other(4)
    kernel_slab(4)
    predict_slab(4)
    for rel in (3, 5, 4):
        join(rel)

    got_y1 = send(q.at[1, :, 1 - yl], ry1, y1_s.at[0], y1_r.at[0], pair_y)
    got_x0 = [
        send(q.at[0, at_x(d)], rx0.at[d - 1], x0_s.at[d - 1], x0_r.at[d - 1], to(dx=d))
        for d in (2, 1, 3)
    ]
    for k in range(2):
        for m in range(4):
            for n in range(rows // 128):
                hi, lo = halves(kf[k, pl.ds(m * 128, 128), lanes(n)].T)
                kth[k, pl.ds(n * 128, 128), lanes(m)] = hi
                ktl[k, pl.ds(n * 128, 128), lanes(m)] = lo
    got_y1.wait_recv()
    for i in range(NX):
        t1[i] = q[1, i, yl] + ry1[i]
    got_x1 = [
        send(t1.at[at_x(d)], rx1.at[d - 1], x1_s.at[d - 1], x1_r.at[d - 1], to(dx=d))
        for d in (2, 1, 3)
    ]
    for copy in got_x0:
        copy.wait_recv()
    for h in range(2):
        s0[h] = (q[0, x, h] + rx0[0, h]) + (rx0[1, h] + rx0[2, h])
    got_y0 = send(s0.at[1 - yl], ry0, y0_s.at[0], y0_r.at[0], pair_y)

    def spread_z(k):
        return [
            send(tz.at[k, at_z(d)], rz.at[k, d - 1], rz_s.at[k, d - 1], rz_r.at[k, d - 1], to(dz=d))
            for d in range(1, NZ)
        ]

    for copy in got_x1:
        copy.wait_recv()
    tz[1] = ((t1[x] + rx1[0]) + (rx1[1] + rx1[2])).reshape(NZ, 16, LANES)
    got_z1 = spread_z(1)
    got_y0.wait_recv()
    tz[0] = (s0[yl] + ry0[...]).reshape(NZ, 16, LANES)
    got_z0 = spread_z(0)

    def residual(k, got):
        for copy in got:
            copy.wait_recv()
        acc = tz[k, z]
        for d in range(1, NZ):
            acc = acc + rz[k, d - 1]
        at = pl.ds(pl.multiple_of(z * 16, 16), 16)
        value = acc[:, :wide] - targ_ref[k]
        rb[k, x, c, yl, at, :] = jnp.zeros((16, LANES), F32)
        rb[k, x, c, yl, at, pl.ds(0, wide)] = value
        block = rb.at[k, x, c, yl, at]
        res_ref[k] = value
        return [
            send(block, block, az_s.at[k, d - 1], az_r.at[k, d - 1], to(dz=d)) for d in range(1, NZ)
        ]

    got_a1 = residual(1, got_z1)
    got_a0 = residual(0, got_z0)

    for copy in got_a1:
        copy.wait_recv()
    part = rb.at[1, x, c, yl]
    got_ax1 = [send(part, part, ax1_s.at[d - 1], ax1_r.at[d - 1], to(dx=d)) for d in (2, 1, 3)]
    for copy in got_a0:
        copy.wait_recv()
    part = rb.at[0, x, c, yl]
    got_ay0 = send(part, part, ay0_s.at[0], ay0_r.at[0], pair_y)
    for copy in got_ax1:
        copy.wait_recv()
    part = rb.at[1, :, c, yl]
    got_ay1 = send(part, part, ay1_s.at[0], ay1_r.at[0], pair_y)
    got_ad = {1: [], 0: []}
    got_ad[1].append(send(part, part, ad_s.at[0], ad_r.at[0], to(flip=True)))
    got_ay0.wait_recv()
    part = rb.at[0, x, c]
    got_ax0 = {
        d: send(part, part, ax0_s.at[d - 1], ax0_r.at[d - 1], to(dx=d)) for d in (2, 1, 3)
    }
    got_ad[0].append(send(part, part, ad_s.at[1], ad_r.at[1], to(flip=True)))
    for d in (1, 3, 2):
        got_ax0[d].wait_recv()
        part = rb.at[0, at_x(NX - d), c]
        got_ad[0].append(send(part, part, ad_s.at[1 + d], ad_r.at[1 + d], to(flip=True)))
    got_ay1.wait_recv()
    part = rb.at[1, :, c, 1 - yl]
    got_ad[1].append(send(part, part, ad_s.at[5], ad_r.at[5], to(flip=True)))

    def gradient(k):
        for copy in got_ad[k]:
            copy.wait_recv()
        for i in range(NX):
            for cc in range(2):
                for h in range(2):
                    hi, lo = halves(rb[k, i, cc, h])
                    for zs in range(NZ):
                        at = pl.ds(zs * 64 + (cc * 2 + h) * 16, 16)
                        rhi[at, lanes(i)] = hi[zs * 16 : zs * 16 + 16]
                        rlo[at, lanes(i)] = lo[zs * 16 : zs * 16 + 16]
        acc = jnp.zeros((8, LANES), F32)
        for n in range(rows // 128):
            at = pl.ds(n * 128, 128)
            kh, kl = kth[k, at, :], ktl[k, at, :]
            out = dot_plain(kl, rhi[...]) + dot_plain(kh, rlo[...]) + dot_plain(kh, rhi[...])
            out = out * (1.0 / (2 * NZ * 2 * 16))
            for i in range(NX):
                v = out[:, i * LANES : (i + 1) * LANES]
                g[k, i, at, :] = v
                acc = acc + jnp.sum((v * v).reshape(16, 8, LANES), axis=0)
        return jnp.sum(acc, axis=0, keepdims=True)

    parts = [gradient(0), gradient(1)]

    line = lax.broadcasted_iota(jnp.int32, (8, LANES), 0)
    acc = jnp.where(line == 0, parts[0], jnp.where(line == 1, parts[1], 0.0))
    pp[0] = acc
    got = [
        send(pp.at[0], pp.at[8 + n], p_s.at[8 + n], p_r.at[8 + n], to(dx, dy))
        for n, (dx, dy) in enumerate(plane)
    ]
    first = pl.ds(0, EARLY)
    got_e = []
    for k, dst in ((0, e0), (1, e1)):
        for d in (2, 1, 3):
            got_e.append(
                send(
                    g.at[k, at_x(d), first], dst.at[d - 1], e_s.at[k, d - 1], e_r.at[k, d - 1],
                    to(dx=d),
                )
            )
    for n, copy in enumerate(got):
        copy.wait_recv()
        acc = acc + pp[8 + n]
    pp[23] = acc
    got = [send(pp.at[23], pp.at[d], p_s.at[d], p_r.at[d], to(dz=d)) for d in range(1, NZ)]
    for d, copy in enumerate(got, 1):
        copy.wait_recv()
        acc = acc + pp[d]
    pp[24] = acc
    got = send(pp.at[24], pp.at[25], p_s.at[0], p_r.at[0], to(flip=True))
    got.wait_recv()
    acc = acc + pp[25]
    sums = jnp.sum(acc, axis=1, keepdims=True)
    factor = [0.1 / jnp.sqrt(sums[k : k + 1] / entries + 1e-6) for k in range(2)]

    late = pl.ds(EARLY, rows - EARLY)
    got = {}
    for d in (2, 1, 3):
        us[d - 1] = g[0, at_x(d), late, :] * factor[0] + g[1, at_x(d), late, :] * factor[1]
        got[d] = send(us.at[d - 1], upd.at[x], u_s.at[d - 1], u_r.at[d - 1], to(dx=d))

    stores = []

    def update(i, early, rest):
        head = pl.ds(pl.multiple_of(i * rows, 8), EARLY)
        coef_ref[head, :] = coef_ref[head, :] - early[:, :wide]
        foot = pl.ds(pl.multiple_of(i * rows + EARLY, 8), rows - EARLY)
        coef_ref[foot, :] = coef_ref[foot, :] - rest[:, :wide]
        store = pltpu.make_async_copy(
            coef_ref.at[slot(i)], new_hbm.at[slot(i)], out_s.at[len(stores)]
        )
        store.start()
        stores.append(store)

    def own(at):
        return g[0, x, at, :] * factor[0] + g[1, x, at, :] * factor[1]

    update(x, own(first), own(late))
    for copy in got_e:
        copy.wait_recv()
    for d in (1, 3, 2):
        early = e0[d - 1] * factor[0] + e1[d - 1] * factor[1]
        got[d].wait_recv()
        i = at_x(NX - d)
        update(i, early, upd[i])
    for store in stores:
        store.wait()
    for copy in sent:
        copy.wait_send()


def body(features, centres, coefs, batch_index, targets):
    total = centres.shape[0]
    rows = total // NX
    entries = total * lax.axis_size(CEN) * coefs.shape[1] * lax.axis_size(OUT)
    vm = lambda *shape: pltpu.VMEM(shape, F32)
    vb = lambda *shape: pltpu.VMEM(shape, BF16)
    dma = lambda *shape: pltpu.SemaphoreType.DMA(shape)
    two = lambda *shape: [dma(*shape), dma(*shape)]
    wide = coefs.shape[1]
    scratch = [
        vm(total, LANES), vm(total, LANES), vm(total, wide), vm(*targets.shape),
        vm(total, LANES), vm(8, 2, 2, 8, 32, LANES), vm(8, rows, LANES), vm(NX, rows, LANES),
        vb(W, rows), vb(W, rows), vb(rows, 512), vb(rows, 512),
        vb(NZ, 128, W), vb(NZ, 128, W), vm(NZ, 128, LANES),
        vm(2, 512, rows), vb(2, rows, 512), vb(2, rows, 512),
        vm(2, 2, 2, 16, 512), vm(NZ, 2, NX, 2, 16, LANES), vm(NZ, 2, NX, 2, 16, LANES),
        vm(2, NX, 2, 128, LANES),
        vm(3, 2, 128, LANES), vm(2, 128, LANES), vm(128, LANES), vm(NX, 128, LANES),
        vm(NX, 128, LANES), vm(3, 128, LANES), vm(2, NZ, 16, LANES), vm(2, 7, 16, LANES),
        vm(2, NX, 2, 2, 128, LANES), vb(512, 512), vb(512, 512),
        vm(2, NX, rows, LANES), vm(3, rows - EARLY, LANES), vm(NX, rows - EARLY, LANES),
        vm(3, EARLY, LANES), vm(3, EARLY, LANES), vm(26, 8, LANES),
        dma(4), *two(15), *two(3), *two(4), *two(3), *two(2, 4, 2), *two(8, 2),
        *two(8), *two(3), *two(1), *two(1), *two(3), *two(2, 7),
        *two(2, 7), *two(1), *two(3), *two(3), *two(1), *two(6),
        *two(23), *two(3), *two(2, 3), dma(4),
    ]
    whole = pl.BlockSpec(memory_space=pltpu.VMEM)
    there = pl.BlockSpec(memory_space=pl.ANY)
    new, resid = pl.pallas_call(
        functools.partial(kernel, float(entries)),
        out_shape=(
            jax.ShapeDtypeStruct(coefs.shape, F32),
            jax.ShapeDtypeStruct(targets.shape, F32),
        ),
        in_specs=[pl.BlockSpec(memory_space=pltpu.SMEM)] + [there] * 4,
        out_specs=(there, whole),
        scratch_shapes=scratch,
        compiler_params=pltpu.CompilerParams(
            collective_id=0, has_side_effects=True, vmem_limit_bytes=60 * 2**20
        ),
        name="step",
    )(batch_index, features, centres, coefs, targets)
    return resid, new


def solution(mesh):
    torus = Mesh(mesh.devices.reshape(2, 8, 2, 4, 2), ("cen_0", "cen_1", "cen_2", "out_0", "out_1"))
    return jax.shard_map(
        body,
        mesh=torus,
        in_specs=(P(CEN, OUT), P(CEN, OUT), P(CEN, OUT), P(None, CEN), P(None, CEN, OUT)),
        out_specs=(P(None, CEN, OUT), P(CEN, OUT)),
        check_vma=False,
    )
```

```python
import functools
import math

import jax
import jax.numpy as jnp
from jax import lax
from jax.experimental import pallas as pl
from jax.experimental.pallas import tpu as pltpu
from jax.sharding import Mesh
from jax.sharding import PartitionSpec as P

W = 1024
LANES = 128
CEN = ("cen_0", "cen_1", "cen_2")
OUT = ("out_0", "out_1")
MESH = pl.DeviceIdType.MESH
NX, NY, NZ = 4, 4, 8
F32, BF16 = jnp.float32, jnp.bfloat16


def halves(v):
    hi = v.astype(BF16)
    return hi, (v - hi.astype(F32)).astype(BF16)


def dot_rows(a, b):
    return lax.dot_general(a, b, (((1,), (1,)), ((), ())), preferred_element_type=F32)


def dot_plain(a, b):
    return lax.dot_general(a, b, (((1,), (0,)), ((), ())), preferred_element_type=F32)


EARLY = 224
FAR_Z = (4, 3, 5, 2, 6, 1, 7)


def kernel(
    entries, idx_hbm, feat_hbm, cen_hbm, coef_hbm, targ_hbm, new_hbm, res_hbm,
    idx_ref, res_ref, feat_ref, cen_ref, coef_ref, targ_ref,
    cpad, bs, cs, gs, cth, ctl, ghi, glo, sbh, sbl, bsq, begun, kf, kth, ktl,
    po, psend, precv, q, rx0, s0, ry0, ry1, t1, rx1, tz, rz, rb, rhi, rlo,
    g, us, upd, e0, e1, pp,
    in_s, pl_s, pl_r, cx_s, cx_r, cy_s, cy_r, gx_s, gx_r, z_s, z_r, d_s, d_r,
    pr_s, pr_r, x0_s, x0_r, y0_s, y0_r, y1_s, y1_r, x1_s, x1_r, rz_s, rz_r,
    az_s, az_r, ay0_s, ay0_r, ax0_s, ax0_r, ax1_s, ax1_r, ay1_s, ay1_r, ad_s, ad_r,
    p_s, p_r, u_s, u_r, e_s, e_r, out_s,
):
    x, yh = lax.axis_index("out_0"), lax.axis_index("out_1")
    yl, z, c = lax.axis_index("cen_0"), lax.axis_index("cen_1"), lax.axis_index("cen_2")
    y = yh * 2 + yl
    rows = cen_ref.shape[0] // NX
    blk = yh * NX + x
    wide = coef_ref.shape[1]

    def at_x(d):
        return lax.rem(x + d, NX)

    def at_z(d):
        return lax.rem(z + d + NZ, NZ)

    def slot(i):
        return pl.ds(pl.multiple_of(i * rows, 8), rows)

    def lanes(i):
        return pl.ds(i * LANES, LANES)

    def to(dx=0, dy=0, dz=0, flip=False):
        ny = lax.rem(y + dy, NY)
        return {
            "out_0": at_x(dx), "out_1": lax.div(ny, 2), "cen_0": lax.rem(ny, 2),
            "cen_1": at_z(dz), "cen_2": 1 - c if flip else c,
        }

    pair_y = {"out_0": x, "out_1": yh, "cen_0": 1 - yl, "cen_1": z, "cen_2": c}
    plane = [(dx, dy) for dx in range(NX) for dy in range(NY) if dx or dy]
    plane.sort(key=lambda p: -(min(p[0], NX - p[0]) + min(p[1], NY - p[1])))
    peers = [to(dx, dy) for dx, dy in plane] + [to(dz=d) for d in range(1, NZ)] + [to(flip=True)]

    loads = [
        pltpu.make_async_copy(src, dst, in_s.at[n])
        for n, (src, dst) in enumerate(
            (
                (feat_hbm, feat_ref), (cen_hbm, cen_ref), (coef_hbm, coef_ref), (targ_hbm, targ_ref),
                (idx_hbm, idx_ref),
            )
        )
    ]
    for load in loads:
        load.start()
    barrier = pltpu.get_barrier_semaphore()
    for peer in peers:
        pl.semaphore_signal(barrier, inc=1, device_id=peer, device_id_type=MESH)

    sent = []

    def send(src, dst, ss, rs, dev):
        copy = pltpu.make_async_remote_copy(
            src_ref=src, dst_ref=dst, send_sem=ss, recv_sem=rs, device_id=dev, device_id_type=MESH
        )
        copy.start()
        sent.append(copy)
        return copy

    mine = bs.at[z, c, yl, blk]
    loads[4].wait()
    loads[0].wait()
    for k in range(2):
        for j in range(16):
            mine[pl.ds(k * 16 + j, 1), :] = feat_ref[pl.ds(idx_ref[k, j], 1), :]
    loads[1].wait()
    cs[blk] = cen_ref[slot(x), :]
    pl.semaphore_wait(barrier, len(peers))

    got_plane = [
        send(mine, mine, pl_s.at[n], pl_r.at[n], to(dx, dy)) for n, (dx, dy) in enumerate(plane)
    ]
    got_cx = {}
    for d in (2, 1, 3):
        got_cx[d] = send(
            cen_ref.at[slot(at_x(d))], cs.at[blk], cx_s.at[d - 1], cx_r.at[d - 1], to(dx=d)
        )
    got_cy = {0: send(cen_ref.at[slot(x)], cs.at[blk], cy_s.at[0], cy_r.at[0], to(dy=2))}

    loads[2].wait()
    loads[3].wait()

    @pl.loop(0, cpad.shape[0] // 256)
    def _(i):
        at = pl.ds(pl.multiple_of(i * 256, 256), 256)
        cpad[at, :] = jnp.zeros((256, LANES), F32)
        cpad[at, pl.ds(0, wide)] = coef_ref[at, :]

    gs[x] = cpad[slot(x), :]

    for copy in got_plane:
        copy.wait_recv()
    got_z, got_d = {}, {}
    for h in range(2):
        part = bs.at[z, c, h]
        for way, dz in ((0, 1), (1, -1)):
            got_z[way, 1, h] = send(part, part, z_s.at[way, 0, h], z_r.at[way, 0, h], to(dz=dz))
    for h in range(2):
        part = bs.at[z, c, h]
        got_d[0, h] = send(part, part, d_s.at[0, h], d_r.at[0, h], to(flip=True))

    def split_rows(zs, cc, h):
        acc = [None, None]
        for b in range(2 * NX):
            for k in range(2):
                v = bs[zs, cc, h, b, pl.ds(k * 16, 16), :]
                hi, lo = halves(v)
                at = pl.ds(pl.multiple_of((k * 4 + cc * 2 + h) * 16, 16), 16)
                sbh[zs, at, lanes(b)] = hi
                sbl[zs, at, lanes(b)] = lo
                acc[k] = v * v if acc[k] is None else acc[k] + v * v
        for k in range(2):
            at = pl.ds(pl.multiple_of((k * 4 + cc * 2 + h) * 16, 16), 16)
            total = jnp.sum(acc[k], axis=1, keepdims=True)
            bsq[zs, at, :] = jnp.broadcast_to(total, (16, LANES))

    def other(rel):
        for h in range(2):
            got_d[rel, h].wait_recv()
            split_rows(at_z(rel), 1 - c, h)

    for h in range(2):
        split_rows(z, c, h)
    for d in (2, 1, 3):
        got_cx[d].wait_recv()
        part = cs.at[yh * NX + at_x(NX - d)]
        got_cy[d] = send(part, part, cy_s.at[d], cy_r.at[d], to(dy=2))
    got_g = [
        send(cpad.at[slot(at_x(d))], gs.at[x], gx_s.at[d - 1], gx_r.at[d - 1], to(dx=d))
        for d in (2, 1, 3)
    ]

    def ring_step(s):
        for h in range(2):
            for way, dz in ((0, 1), (1, -1)):
                if s == 4 and h != way:
                    continue
                got_z[way, s, h].wait_recv()
                part = bs.at[at_z(-dz * s), c, h]
                if s < 3 or (s == 3 and h == way):
                    got_z[way, s + 1, h] = send(
                        part, part, z_s.at[way, s, h], z_r.at[way, s, h], to(dz=dz)
                    )
                rel = (-dz * s) % NZ
                got_d[rel, h] = send(part, part, d_s.at[rel, h], d_r.at[rel, h], to(flip=True))
        for h in range(2):
            for way, dz in ((0, 1), (1, -1)):
                if s < 4 or h == way:
                    split_rows(at_z(-dz * s), c, h)

    def take_centres(base):
        squares = None
        for i in range(NX):
            v = cs[base + i].T
            hi, lo = halves(v)
            at = pl.ds(pl.multiple_of((base + i) * LANES, LANES), LANES)
            cth[at, :] = hi
            ctl[at, :] = lo
            squares = v * v if squares is None else squares + v * v
        return jnp.sum(squares, axis=0, keepdims=True)

    def products(zs, part, cat):
        at = pl.ds(pl.multiple_of(part * NX * LANES, LANES), NX * LANES)
        bh, bl = sbh[zs, :, at], sbl[zs, :, at]
        ch, cl = cth[at, cat], ctl[at, cat]
        return (dot_plain(bl, cl) + dot_plain(bl, ch)) + dot_plain(bh, cl) + dot_plain(bh, ch)

    def begin_slab(rel):
        zs = at_z(rel)
        for n in range(rows // 256):
            cat = pl.ds(n * 256, 256)
            begun[zs, :, cat] = products(zs, yh, cat)

    first_sq = take_centres(yh * NX)
    ring_step(1)
    other(0)
    ring_step(2)
    for rel in (1, 7):
        other(rel)
    for rel in (0, 1, 7):
        begin_slab(rel)
    ring_step(3)
    for rel in (2, 6):
        other(rel)
        begin_slab(rel)
    for d in (0, 1, 3, 2):
        got_cy[d].wait_recv()
    centre_sq = first_sq + take_centres((1 - yh) * NX)

    def kernel_slab(rel):
        zs = at_z(rel)
        square = bsq[zs]
        for n in range(rows // 256):
            cat = pl.ds(n * 256, 256)
            inner = begun[zs, :, cat] + products(zs, 1 - yh, cat)
            for i in range(2):
                lo = i * LANES
                sums = square + centre_sq[:, n * 256 + lo : n * 256 + lo + LANES]
                sq = sums - 2.0 * inner[:, lo : lo + LANES]
                kern = jnp.exp(jnp.sqrt(jnp.maximum(sq, 0.0)) * (-1.0 / (0.5 * math.sqrt(W))))
                for k in range(2):
                    at = pl.ds(pl.multiple_of(zs * 64, 64), 64)
                    kf[k, at, pl.ds(n * 256 + lo, LANES)] = kern[k * 64 : k * 64 + 64]

    got_p = {}

    def predict_slab(rel):
        zs = at_z(rel)
        at = pl.ds(pl.multiple_of(zs * 64, 64), 64)
        kh, kl = halves(jnp.concatenate([kf[0, at, :], kf[1, at, :]], axis=0))
        out = dot_plain(kl, ghi[...]) + dot_plain(kh, glo[...]) + dot_plain(kh, ghi[...])
        po[...] = out.reshape(2, 2, 2, 16, NX * LANES)
        zat = pl.ds(pl.multiple_of(zs * 16, 16), 16)
        for k in range(2):
            for h in range(2):
                for i in range(NX):
                    psend[zs, k, i, h] = po[k, 1 - c, h, :, lanes(i)]
        for k in range(2):
            for h in range(2):
                for i in range(NX):
                    q[k, i, h, zat, :] = po[k, c, h, :, lanes(i)]
        got_p[rel] = send(psend.at[zs], precv.at[zs], pr_s.at[rel], pr_r.at[rel], to(flip=True))

    def join(rel):
        got_p[rel].wait_recv()
        zs = at_z(rel)
        zat = pl.ds(pl.multiple_of(zs * 16, 16), 16)
        for k in range(2):
            for h in range(2):
                for i in range(NX):
                    q[k, i, h, zat, :] = q[k, i, h, zat, :] + precv[zs, k, i, h]

    for rel in (0, 1, 7, 2, 6):
        kernel_slab(rel)
    for copy in got_g:
        copy.wait_recv()
    for i in range(NX):
        hi, lo = halves(gs[i])
        ghi[:, lanes(i)] = hi
        glo[:, lanes(i)] = lo
    for rel in (3, 5):
        other(rel)
        begin_slab(rel)
        kernel_slab(rel)
    ready = (0, 1, 7, 2, 6, 3, 5)
    for rel in ready:
        predict_slab(rel)
    ring_step(4)
    for rel in ready[:-2]:
        join(rel)
    other(4)
    begin_slab(4)
    kernel_slab(4)
    predict_slab(4)
    for rel in (3, 5, 4):
        join(rel)

    got_y1 = send(q.at[1, :, 1 - yl], ry1, y1_s.at[0], y1_r.at[0], pair_y)
    got_x0 = [
        send(q.at[0, at_x(d)], rx0.at[d - 1], x0_s.at[d - 1], x0_r.at[d - 1], to(dx=d))
        for d in (2, 1, 3)
    ]
    for k in range(2):
        for m in range(4):
            for n in range(rows // 128):
                hi, lo = halves(kf[k, pl.ds(m * 128, 128), lanes(n)].T)
                kth[k, pl.ds(n * 128, 128), lanes(m)] = hi
                ktl[k, pl.ds(n * 128, 128), lanes(m)] = lo
    got_y1.wait_recv()
    for i in range(NX):
        t1[i] = q[1, i, yl] + ry1[i]
    got_x1 = [
        send(t1.at[at_x(d)], rx1.at[d - 1], x1_s.at[d - 1], x1_r.at[d - 1], to(dx=d))
        for d in (2, 1, 3)
    ]
    for copy in got_x0:
        copy.wait_recv()
    for h in range(2):
        s0[h] = (q[0, x, h] + rx0[0, h]) + (rx0[1, h] + rx0[2, h])
    got_y0 = send(s0.at[1 - yl], ry0, y0_s.at[0], y0_r.at[0], pair_y)

    def spread_z(k):
        return [
            send(tz.at[k, at_z(d)], rz.at[k, d - 1], rz_s.at[k, d - 1], rz_r.at[k, d - 1], to(dz=d))
            for d in FAR_Z
        ]

    for copy in got_x1:
        copy.wait_recv()
    tz[1] = ((t1[x] + rx1[0]) + (rx1[1] + rx1[2])).reshape(NZ, 16, LANES)
    got_z1 = spread_z(1)
    got_y0.wait_recv()
    tz[0] = (s0[yl] + ry0[...]).reshape(NZ, 16, LANES)
    got_z0 = spread_z(0)

    def residual(k, got):
        for copy in got:
            copy.wait_recv()
        acc = tz[k, z]
        for d in range(1, NZ):
            acc = acc + rz[k, d - 1]
        at = pl.ds(pl.multiple_of(z * 16, 16), 16)
        value = acc[:, :wide] - targ_ref[k]
        rb[k, x, c, yl, at, :] = jnp.zeros((16, LANES), F32)
        rb[k, x, c, yl, at, pl.ds(0, wide)] = value
        block = rb.at[k, x, c, yl, at]
        res_ref[k] = value
        return [
            send(block, block, az_s.at[k, d - 1], az_r.at[k, d - 1], to(dz=d)) for d in FAR_Z
        ]

    got_a1 = residual(1, got_z1)
    got_a0 = residual(0, got_z0)
    keep = pltpu.make_async_copy(res_ref, res_hbm, in_s.at[5])
    keep.start()

    for copy in got_a1:
        copy.wait_recv()
    part = rb.at[1, x, c, yl]
    got_ax1 = [send(part, part, ax1_s.at[d - 1], ax1_r.at[d - 1], to(dx=d)) for d in (2, 1, 3)]
    for copy in got_a0:
        copy.wait_recv()
    part = rb.at[0, x, c, yl]
    got_ay0 = send(part, part, ay0_s.at[0], ay0_r.at[0], pair_y)
    for copy in got_ax1:
        copy.wait_recv()
    part = rb.at[1, :, c, yl]
    got_ay1 = send(part, part, ay1_s.at[0], ay1_r.at[0], pair_y)
    got_ad = {1: [], 0: []}
    got_ad[1].append(send(part, part, ad_s.at[0], ad_r.at[0], to(flip=True)))
    got_ay0.wait_recv()
    part = rb.at[0, x, c]
    got_ax0 = {
        d: send(part, part, ax0_s.at[d - 1], ax0_r.at[d - 1], to(dx=d)) for d in (2, 1, 3)
    }
    got_ad[0].append(send(part, part, ad_s.at[1], ad_r.at[1], to(flip=True)))
    for d in (1, 3, 2):
        got_ax0[d].wait_recv()
        part = rb.at[0, at_x(NX - d), c]
        got_ad[0].append(send(part, part, ad_s.at[1 + d], ad_r.at[1 + d], to(flip=True)))
    got_ay1.wait_recv()
    part = rb.at[1, :, c, 1 - yl]
    got_ad[1].append(send(part, part, ad_s.at[5], ad_r.at[5], to(flip=True)))

    def gradient(k):
        for copy in got_ad[k]:
            copy.wait_recv()
        for i in range(NX):
            for cc in range(2):
                for h in range(2):
                    hi, lo = halves(rb[k, i, cc, h])
                    for zs in range(NZ):
                        at = pl.ds(zs * 64 + (cc * 2 + h) * 16, 16)
                        rhi[at, lanes(i)] = hi[zs * 16 : zs * 16 + 16]
                        rlo[at, lanes(i)] = lo[zs * 16 : zs * 16 + 16]
        acc = jnp.zeros((8, LANES), F32)
        for n in range(rows // 128):
            at = pl.ds(n * 128, 128)
            kh, kl = kth[k, at, :], ktl[k, at, :]
            out = dot_plain(kl, rhi[...]) + dot_plain(kh, rlo[...]) + dot_plain(kh, rhi[...])
            out = out * (1.0 / (2 * NZ * 2 * 16))
            for i in range(NX):
                v = out[:, i * LANES : (i + 1) * LANES]
                g[k, i, at, :] = v
                acc = acc + jnp.sum((v * v).reshape(16, 8, LANES), axis=0)
        return jnp.sum(acc, axis=0, keepdims=True)

    parts = [gradient(0), gradient(1)]

    line = lax.broadcasted_iota(jnp.int32, (8, LANES), 0)
    acc = jnp.where(line == 0, parts[0], jnp.where(line == 1, parts[1], 0.0))
    pp[0] = acc
    got = [
        send(pp.at[0], pp.at[8 + n], p_s.at[8 + n], p_r.at[8 + n], to(dx, dy))
        for n, (dx, dy) in enumerate(plane)
    ]
    first = pl.ds(0, EARLY)
    got_e = []
    for k, dst in ((0, e0), (1, e1)):
        for d in (2, 1, 3):
            got_e.append(
                send(
                    g.at[k, at_x(d), first], dst.at[d - 1], e_s.at[k, d - 1], e_r.at[k, d - 1],
                    to(dx=d),
                )
            )
    for n, copy in enumerate(got):
        copy.wait_recv()
        acc = acc + pp[8 + n]
    pp[23] = acc
    got = [send(pp.at[23], pp.at[d], p_s.at[d], p_r.at[d], to(dz=d)) for d in FAR_Z]
    for d, copy in zip(FAR_Z, got):
        copy.wait_recv()
        acc = acc + pp[d]
    pp[24] = acc
    got = send(pp.at[24], pp.at[25], p_s.at[0], p_r.at[0], to(flip=True))
    got.wait_recv()
    acc = acc + pp[25]
    sums = jnp.sum(acc, axis=1, keepdims=True)
    factor = [0.1 / jnp.sqrt(sums[k : k + 1] / entries + 1e-6) for k in range(2)]

    late = pl.ds(EARLY, rows - EARLY)
    got = {}
    for d in (2, 1, 3):
        us[d - 1] = g[0, at_x(d), late, :] * factor[0] + g[1, at_x(d), late, :] * factor[1]
        got[d] = send(us.at[d - 1], upd.at[x], u_s.at[d - 1], u_r.at[d - 1], to(dx=d))

    stores = []

    def update(i, early, rest):
        head = pl.ds(pl.multiple_of(i * rows, 8), EARLY)
        coef_ref[head, :] = coef_ref[head, :] - early[:, :wide]
        foot = pl.ds(pl.multiple_of(i * rows + EARLY, 8), rows - EARLY)
        coef_ref[foot, :] = coef_ref[foot, :] - rest[:, :wide]
        store = pltpu.make_async_copy(
            coef_ref.at[slot(i)], new_hbm.at[slot(i)], out_s.at[len(stores)]
        )
        store.start()
        stores.append(store)

    def own(at):
        return g[0, x, at, :] * factor[0] + g[1, x, at, :] * factor[1]

    update(x, own(first), own(late))
    for copy in got_e:
        copy.wait_recv()
    for d in (1, 3, 2):
        early = e0[d - 1] * factor[0] + e1[d - 1] * factor[1]
        got[d].wait_recv()
        i = at_x(NX - d)
        update(i, early, upd[i])
    for store in stores:
        store.wait()
    keep.wait()
    for copy in sent:
        copy.wait_send()


def body(features, centres, coefs, batch_index, targets):
    total = centres.shape[0]
    rows = total // NX
    entries = total * lax.axis_size(CEN) * coefs.shape[1] * lax.axis_size(OUT)
    vm = lambda *shape: pltpu.VMEM(shape, F32)
    vb = lambda *shape: pltpu.VMEM(shape, BF16)
    dma = lambda *shape: pltpu.SemaphoreType.DMA(shape)
    two = lambda *shape: [dma(*shape), dma(*shape)]
    wide = coefs.shape[1]
    scratch = [
        pltpu.SMEM(batch_index.shape, jnp.int32), vm(*targets.shape),
        vm(total, LANES), vm(total, LANES), vm(total, wide), vm(*targets.shape),
        vm(total, LANES), vm(8, 2, 2, 8, 32, LANES), vm(8, rows, LANES), vm(NX, rows, LANES),
        vb(W, rows), vb(W, rows), vb(rows, 512), vb(rows, 512),
        vb(NZ, 128, W), vb(NZ, 128, W), vm(NZ, 128, LANES),
        vm(NZ, 128, rows), vm(2, 512, rows), vb(2, rows, 512), vb(2, rows, 512),
        vm(2, 2, 2, 16, 512), vm(NZ, 2, NX, 2, 16, LANES), vm(NZ, 2, NX, 2, 16, LANES),
        vm(2, NX, 2, 128, LANES),
        vm(3, 2, 128, LANES), vm(2, 128, LANES), vm(128, LANES), vm(NX, 128, LANES),
        vm(NX, 128, LANES), vm(3, 128, LANES), vm(2, NZ, 16, LANES), vm(2, 7, 16, LANES),
        vm(2, NX, 2, 2, 128, LANES), vb(512, 512), vb(512, 512),
        vm(2, NX, rows, LANES), vm(3, rows - EARLY, LANES), vm(NX, rows - EARLY, LANES),
        vm(3, EARLY, LANES), vm(3, EARLY, LANES), vm(26, 8, LANES),
        dma(6), *two(15), *two(3), *two(4), *two(3), *two(2, 4, 2), *two(8, 2),
        *two(8), *two(3), *two(1), *two(1), *two(3), *two(2, 7),
        *two(2, 7), *two(1), *two(3), *two(3), *two(1), *two(6),
        *two(23), *two(3), *two(2, 3), dma(4),
    ]
    there = pl.BlockSpec(memory_space=pl.ANY)
    new, resid = pl.pallas_call(
        functools.partial(kernel, float(entries)),
        out_shape=(
            jax.ShapeDtypeStruct(coefs.shape, F32),
            jax.ShapeDtypeStruct(targets.shape, F32),
        ),
        in_specs=[there] * 5,
        out_specs=(there, there),
        scratch_shapes=scratch,
        compiler_params=pltpu.CompilerParams(
            collective_id=0, has_side_effects=True, vmem_limit_bytes=60 * 2**20
        ),
        name="step",
    )(batch_index, features, centres, coefs, targets)
    return resid, new


def solution(mesh):
    torus = Mesh(mesh.devices.reshape(2, 8, 2, 4, 2), ("cen_0", "cen_1", "cen_2", "out_0", "out_1"))
    return jax.shard_map(
        body,
        mesh=torus,
        in_specs=(P(CEN, OUT), P(CEN, OUT), P(CEN, OUT), P(None, CEN), P(None, CEN, OUT)),
        out_specs=(P(None, CEN, OUT), P(CEN, OUT)),
        check_vma=False,
    )
```
